32 devices in a mesh: slab: 8 (over y, x, core), cross: 4 (over z).
Axes of the slice: x: 2, y: 2, z: 4, core: 2. Of those that a mesh axis runs over, the one named last changes fastest.
Arguments:
- populations: float32 [19, 32, 32, 128], P(None, 'slab', 'cross'), may hold values from 0 to 1, as said below
- fluid_mask: int32 [32, 32, 128], P('slab', 'cross'), may hold values 0 or 1
- relaxation: float32 [32, 32, 128], P('slab', 'cross'), may hold values from 0.8 to 1.7
- positions: int32 [3, 128, 642], P(None, 'slab'), may hold values from -1 to 127, as said below
- triangles: int32 [3, 1280], replicated, may hold values from 0 to 641, as said below
- tension: float32 [128, 1280], P('slab'), may hold values from 0.0003 to 0.003
- coarse_moments: float32 [4, 4096], P(None, 'slab'), may hold values from -0.2 to 1.2, as said below
- interface: int32 [3, 4096], P(None, ('slab', 'cross')), may hold values from -1 to 4095, as said below
Outputs:
- populations_next: float32 [19, 32, 32, 128], P(None, 'slab', 'cross')
- flow: float32 [3, 32, 32, 128], P(None, 'slab', 'cross')
The draws below stay inside these ranges and needn't reach their ends.
Inputs may be any that keep to these rules, and one draw needn't show every extreme that they name: `positions`: nodes of membrane m lie in planes 4 * (m // 16) - 1 to 4 * (m // 16) + 4, columns 0 to 31 and rows 0 to 127. `triangles`: each triangle names three different nodes of a membrane. `interface`: in each block of 128 columns (one device's, slab major), row 0 names different cells of that device's block, numbered (plane * 8 + column) * 128 + row, or -1 for an unused slot; rows 1 and 2 name coarse cells. `populations`: populations are positive. `coarse_moments`: row 0 is a positive density, rows 1 to 3 a velocity.
All inputs are finite; a program needn't handle non-finite values. No bound on the sum of `fluid_mask` on one device may be relied on, other than what follows from the above.
Results may differ from the reference program's by a relative error of at most 0.0001.
Values sent between devices are 32-bit elements; how exact they have to be, the bound alone decides.
A program may use at most 128 MiB of HBM per device.

```python
import math
import jax
import jax.numpy as jnp
import numpy as np
from jax import lax

PL = 4
SX = 8
NY = 128
MEMB_DEV = 16
MNODES = 642
MTRI = 1280
IF_DEV = 128
STEPS = 4
NZ = 32
NX = 32
MEMBS = 128
NCOARSE = 4096
IFACES = 4096


LATTICE_VECTORS = [(0, 0, 0), (1, 0, 0), (-1, 0, 0), (0, 1, 0), (0, -1, 0), (0, 0, 1), (0, 0, -1), (1, 1, 0), (-1, -1, 0), (1, -1, 0), (-1, 1, 0), (1, 0, 1), (-1, 0, -1), (1, 0, -1), (-1, 0, 1), (0, 1, 1), (0, -1, -1), (0, 1, -1), (0, -1, 1)]


LATTICE_WEIGHTS = [1.0 / 3.0] + [1.0 / 18.0] * 6 + [1.0 / 36.0] * 12


def equilibrium_draw(density, velocity):
    squared = velocity[0] * velocity[0] + velocity[1] * velocity[1] + velocity[2] * velocity[2]
    planes = []
    for member, vector in enumerate(LATTICE_VECTORS):
        projected = vector[0] * velocity[0] + vector[1] * velocity[1] + vector[2] * velocity[2]
        planes.append(LATTICE_WEIGHTS[member] * density * (1.0 + 3.0 * projected + 4.5 * projected * projected - 1.5 * squared))
    return jnp.stack(planes)


def draw_populations(key, part):
    subkeys = jax.random.split(jax.random.fold_in(key, 3), 3)
    grid = (NZ, NX, NY)
    density = jax.random.uniform(subkeys[0], grid, jnp.float32, 0.9, 1.1)
    velocity = jnp.clip(0.05 * jax.random.normal(subkeys[1], (3,) + grid, jnp.float32), -0.15, 0.15)
    spread = 0.1
    noise = jax.random.uniform(subkeys[2], (19,) + grid, jnp.float32, -1.0, 1.0)
    return equilibrium_draw(density, velocity) * (1.0 + spread * noise)


def draw_coarse_moments(key, part):
    subkeys = jax.random.split(jax.random.fold_in(key, 4), 2)
    density = jax.random.uniform(subkeys[0], (1, NCOARSE), jnp.float32, 0.9, 1.1)
    velocity = jnp.clip(0.05 * jax.random.normal(subkeys[1], (3, NCOARSE), jnp.float32), -0.15, 0.15)
    return jnp.concatenate([density, velocity], axis=0)


def draw_positions(key, part):
    subkeys = jax.random.split(jax.random.fold_in(key, 5), 5)
    membrane = jnp.arange(MEMBS, dtype=jnp.int32)[:, None]
    slab_owner = membrane // MEMB_DEV
    plane_ids = slab_owner * PL - 1 + jax.random.randint(subkeys[0], (MEMBS, MNODES), 0, PL + 2)
    centre_column = jax.random.randint(subkeys[1], (MEMBS, 1), 3, NX - 3)
    column_ids = jnp.clip(centre_column + jax.random.randint(subkeys[2], (MEMBS, MNODES), -3, 4), 0, NX - 1)
    centre_row = jax.random.randint(subkeys[3], (MEMBS, 1), 3, NY - 3)
    row_ids = centre_row + jax.random.randint(subkeys[4], (MEMBS, MNODES), -3, 4)
    return jnp.stack([plane_ids, column_ids, row_ids]).astype(jnp.int32)


def draw_triangles(key, part):
    subkeys = jax.random.split(jax.random.fold_in(key, 7), 3)
    vertex_one = jax.random.randint(subkeys[0], (MTRI,), 0, MNODES)
    step_one = jax.random.randint(subkeys[1], (MTRI,), 1, MNODES)
    step_two = jax.random.randint(subkeys[2], (MTRI,), 1, MNODES - 1)
    step_two = step_two + (step_two >= step_one).astype(jnp.int32)
    return jnp.stack([vertex_one, (vertex_one + step_one) % MNODES, (vertex_one + step_two) % MNODES]).astype(jnp.int32)


def draw_interface(key, part):
    subkeys = jax.random.split(jax.random.fold_in(key, 9), 5)
    devices = IFACES // IF_DEV
    cell_total = PL * SX * NY

    def choose_cells(device_key):
        return jax.random.permutation(device_key, cell_total)[:IF_DEV]
    chosen = jax.vmap(choose_cells)(jax.random.split(subkeys[0], devices))
    counts = jax.random.randint(subkeys[1], (devices,), max(IF_DEV // 4, 1), IF_DEV + 1)
    fullest = jax.random.randint(subkeys[2], (), 0, devices)
    counts = jnp.where(jnp.arange(devices, dtype=jnp.int32) == fullest, IF_DEV, counts)
    slots = jnp.arange(IF_DEV, dtype=jnp.int32)
    cell_ids = jnp.where(slots[None, :] < counts[:, None], chosen, -1).reshape(-1)
    coarse_one = jax.random.randint(subkeys[3], (IFACES,), 0, NCOARSE)
    coarse_two = jax.random.randint(subkeys[4], (IFACES,), 0, NCOARSE)
    return jnp.stack([cell_ids, coarse_one, coarse_two]).astype(jnp.int32)


def touch_ends(entries, stream_key, least, high):
    longest = entries.shape.index(max(entries.shape))
    spots = []
    for shift in (0, 1):
        where = [jax.random.randint(jax.random.fold_in(stream_key, axis), (), 0, length) for axis, length in enumerate(entries.shape)]
        where[longest] = (where[longest] + shift) % entries.shape[longest]
        spots.append(tuple(where))
    return entries.at[spots[0]].set(least).at[spots[1]].set(high)


def steps_of(rng, extent, shards, smallest, top_value):
    def one(axis_at, blocks):
        heights = jax.random.uniform(jax.random.fold_in(jax.random.fold_in(rng, 6), axis_at), (blocks,), jnp.float32, smallest / len(shards), top_value / len(shards))
        return jnp.repeat(jnp.exp(heights), extent[axis_at] // blocks).reshape((-1,) + (1,) * (len(extent) - axis_at - 1))

    gain = one(*shards[0])
    for cut in shards[1:]:
        gain = gain * one(*cut)
    return gain


def setup_inputs(seed: int = 0) -> dict:
    streams_of = jax.random.split(jax.random.key(seed), 9)
    populations = draw_populations(jax.random.fold_in(streams_of[8], 71), 0)
    fluid_mask = touch_ends((jax.random.randint(streams_of[1], (NZ, NX, NY), 0, 8) < 7).astype(jnp.int32), jax.random.fold_in(streams_of[1], 1), 0, 1)
    relaxation = jnp.clip(jnp.exp(math.log(1.7) - 0.75377182 * jax.random.uniform(streams_of[2], (NZ, NX, NY), jnp.float32) ** steps_of(streams_of[2], (NZ, NX, NY), ((0, 8), (1, 4)), -0.2, 0.2)), 0.8, 1.7)
    positions = draw_positions(jax.random.fold_in(streams_of[8], 71), 0)
    triangles = draw_triangles(jax.random.fold_in(streams_of[8], 71), 0)
    tension = jnp.clip(jnp.exp(math.log(0.003) - 2.3025851 * jax.random.uniform(streams_of[5], (MEMBS, MTRI), jnp.float32) ** steps_of(streams_of[5], (MEMBS, MTRI), ((0, 8),), -0.2, 0.2)), 0.0003, 0.003)
    coarse_moments = draw_coarse_moments(jax.random.fold_in(streams_of[8], 71), 0)
    interface = draw_interface(jax.random.fold_in(streams_of[8], 71), 0)
    return {"populations": populations, "fluid_mask": fluid_mask, "relaxation": relaxation, "positions": positions, "triangles": triangles, "tension": tension, "coarse_moments": coarse_moments, "interface": interface}


LATTICE_VECTORS = [(0, 0, 0), (1, 0, 0), (-1, 0, 0), (0, 1, 0), (0, -1, 0), (0, 0, 1), (0, 0, -1), (1, 1, 0), (-1, -1, 0), (1, -1, 0), (-1, 1, 0), (1, 0, 1), (-1, 0, -1), (1, 0, -1), (-1, 0, 1), (0, 1, 1), (0, -1, -1), (0, 1, -1), (0, -1, 1)]
LATTICE_WEIGHTS = [1.0 / 3.0] + [1.0 / 18.0] * 6 + [1.0 / 36.0] * 12
OPPOSITE = [0] + [member + 1 if member % 2 == 1 else member - 1 for member in range(1, 19)]
ROOT_THREE = math.sqrt(3.0)

def equilibrium(density, velocity):
    lattice = jnp.asarray(LATTICE_VECTORS, jnp.float32)
    weights = jnp.asarray(LATTICE_WEIGHTS, jnp.float32).reshape((19,) + (1,) * density.ndim)
    projected = jnp.einsum('qk,k...->q...', lattice, velocity, precision=lax.Precision.HIGHEST)
    squared = lax.optimization_barrier(jnp.sum(velocity * velocity, axis=0))
    return weights * density * (1.0 + 3.0 * projected + 4.5 * projected * projected - 1.5 * squared)

def moments(fields):
    lattice = jnp.asarray(LATTICE_VECTORS, jnp.float32)
    density = lax.optimization_barrier(jnp.sum(fields, axis=0))
    momentum = jnp.einsum('qk,q...->k...', lattice, fields, precision=lax.Precision.HIGHEST)
    return (density, momentum)

def collide(fields, body_force, relaxation, fluid_mask):
    density, momentum = moments(fields)
    shifted = momentum / density + body_force / (relaxation * density)
    relaxed = fields + relaxation * (equilibrium(density, shifted) - fields)
    reversed_fields = fields[np.array(OPPOSITE)]
    return jnp.where(fluid_mask[None] == 1, relaxed, reversed_fields)

def stream(padded, plane_count, column_count):
    wrapped = jnp.concatenate([padded[..., -1:], padded, padded[..., :1]], axis=-1)
    across = padded.shape[-1]
    planes = []
    for member, vector in enumerate(LATTICE_VECTORS):
        step_plane, step_column, step_row = vector
        planes.append(wrapped[member, 1 - step_plane:1 - step_plane + plane_count, 1 - step_column:1 - step_column + column_count, 1 - step_row:1 - step_row + across])
    return jnp.stack(planes)

def node_force(positions, triangles, tension):
    coords = positions.astype(jnp.float32)
    vertex_one = coords[:, :, triangles[0]]
    vertex_two = coords[:, :, triangles[1]]
    vertex_three = coords[:, :, triangles[2]]
    scaled = tension[None]
    running = jnp.zeros(coords.shape, jnp.float32)
    running = running.at[:, :, triangles[0]].add(scaled * (vertex_two + vertex_three - 2.0 * vertex_one))
    running = running.at[:, :, triangles[1]].add(scaled * (vertex_one + vertex_three - 2.0 * vertex_two))
    running = running.at[:, :, triangles[2]].add(scaled * (vertex_one + vertex_two - 2.0 * vertex_three))
    return running

def spread_global(positions, nodal_force):
    force_field = jnp.zeros((3, NZ + 4, NX + 2, NY), jnp.float32)
    kernel = (0.25, 0.5, 0.25)
    for offset_plane in (-1, 0, 1):
        for offset_column in (-1, 0, 1):
            for offset_row in (-1, 0, 1):
                weight = kernel[offset_plane + 1] * kernel[offset_column + 1] * kernel[offset_row + 1]
                plane_ids = positions[0] + 2 + offset_plane
                column_ids = positions[1] + 1 + offset_column
                row_ids = (positions[2] + offset_row) % NY
                force_field = force_field.at[:, plane_ids, column_ids, row_ids].add(weight * nodal_force)
    return force_field[:, 2:NZ + 2, 1:NX + 1]

def reference(populations, fluid_mask, relaxation, positions, triangles, tension, coarse_moments, interface):
    body_force = spread_global(positions, node_force(positions, triangles, tension))
    blended = 0.75 * coarse_moments[:, interface[1]] + 0.25 * coarse_moments[:, interface[2]]
    boundary = equilibrium(blended[0], blended[1:4])
    local_cell = interface[0]
    device = jnp.arange(IFACES, dtype=jnp.int32) // IF_DEV
    crosses = NX // SX
    slab_owner = device // crosses
    cross_owner = device % crosses
    plane_ids = slab_owner * PL + local_cell // (SX * NY)
    column_ids = cross_owner * SX + local_cell // NY % SX
    row_ids = local_cell % NY
    target = jnp.where(local_cell >= 0, (plane_ids * NX + column_ids) * NY + row_ids, NZ * NX * NY).astype(jnp.int32)
    fields = populations
    for iteration in range(STEPS):
        relaxed = collide(fields, body_force, relaxation, fluid_mask)
        padded = jnp.pad(relaxed, ((0, 0), (1, 1), (1, 1), (0, 0)))
        passed = stream(padded, NZ, NX)
        fields = passed.reshape(19, -1).at[:, target].set(boundary, mode='drop').reshape(passed.shape)
    density, momentum = moments(fields)
    return (fields, ROOT_THREE * momentum / density)
```

```python
import functools
import math

import jax
import jax.numpy as jnp
from jax import lax
from jax.experimental import pallas as pl
from jax.experimental.pallas import tpu as pltpu
from jax.sharding import PartitionSpec as P

STEPS = 4
MESH = pl.DeviceIdType.MESH
LATTICE_VECTORS = [
    (0, 0, 0),
    (1, 0, 0),
    (-1, 0, 0),
    (0, 1, 0),
    (0, -1, 0),
    (0, 0, 1),
    (0, 0, -1),
    (1, 1, 0),
    (-1, -1, 0),
    (1, -1, 0),
    (-1, 1, 0),
    (1, 0, 1),
    (-1, 0, -1),
    (1, 0, -1),
    (-1, 0, 1),
    (0, 1, 1),
    (0, -1, -1),
    (0, 1, -1),
    (0, -1, 1),
]
LATTICE_WEIGHTS = [1.0 / 3.0] + [1.0 / 18.0] * 6 + [1.0 / 36.0] * 12
OPPOSITE = [0] + [q + 1 if q % 2 == 1 else q - 1 for q in range(1, 19)]
ROOT_THREE = math.sqrt(3.0)
DIRECTIONS = [(1, 0), (-1, 0), (0, 1), (0, -1), (1, 1), (-1, -1), (1, -1), (-1, 1)]
NT = (((1,), (1,)), ((), ()))
F32, BF16, I32 = jnp.float32, jnp.bfloat16, jnp.int32


def round_up(value, unit):
    return (value + unit - 1) // unit * unit


def split(value, parts):
    pieces = []
    for _ in range(parts):
        piece = value.astype(BF16).astype(F32)
        pieces.append(piece)
        value = value - piece
    return pieces


def nodal_stage(plane_count, columns, rows, pos_ref, tri_ref, ten_ref, xs, inc, force):
    dims, membranes, nodes = pos_ref.shape
    padded = xs.shape[2]
    triangles = tri_ref.shape[1]
    slab = lax.axis_index("slab")
    cross = lax.axis_index("cross")

    xs[...] = jnp.zeros_like(xs)
    xs[0, :, :nodes] = (pos_ref[0] - slab * plane_count).astype(F32)
    xs[1, :, :nodes] = (pos_ref[1] - cross * columns).astype(F32)
    xs[2, :, :nodes] = (pos_ref[2] - rows // 2).astype(F32)

    corners = [tri_ref[pl.ds(corner, 1), :] for corner in range(3)]
    chunk = 128

    @pl.loop(0, padded // chunk)
    def _(i):
        ids = lax.broadcasted_iota(I32, (chunk, triangles), 0) + i * chunk
        hit = (ids == corners[0]) | (ids == corners[1]) | (ids == corners[2])
        inc[pl.ds(pl.multiple_of(i * chunk, chunk), chunk), :] = jnp.where(hit, 1.0, 0.0).astype(BF16)

    coords = xs[...].reshape(dims * membranes, padded)
    sums = jnp.dot(coords.astype(BF16), inc[...], preferred_element_type=F32)
    tension = ten_ref[...]
    terms = jnp.concatenate(
        [sums[k * membranes : (k + 1) * membranes] * tension for k in range(3)] + [tension], axis=0
    )
    stacked = jnp.concatenate(split(terms, 3), axis=0).astype(BF16)
    gathered = lax.dot_general(stacked, inc[...], NT, preferred_element_type=F32)
    count = terms.shape[0]
    total = gathered[:count] + (gathered[count : 2 * count] + gathered[2 * count :])
    weight = total[3 * membranes :]
    for k in range(3):
        force[k] = total[k * membranes : (k + 1) * membranes] - 3.0 * xs[k] * weight


def spread_stage(xs, force, acc, out_ref):
    _, membranes, padded = xs.shape
    _, planes, columns, rows = out_ref.shape
    plane_count = planes - 4
    half = (columns + 2) // 2
    cells = acc.shape[0] // 6
    acc[...] = jnp.zeros_like(acc)
    unroll = 4 if membranes % 4 == 0 else 1

    @pl.loop(0, membranes // unroll)
    def _(i):
        running = None
        for inner in range(unroll):
            m = pl.ds(i * unroll + inner, 1)
            plane = xs[0, m, :].astype(I32) + 1
            column = xs[1, m, :].astype(I32) + 1
            row = xs[2, m, :].astype(I32) + rows // 2
            inside = (column >= 0) & (column < 2 * half)
            upper = column >= half
            cell = plane * half + jnp.where(upper, column - half, column)
            cell = jnp.where(inside, cell, -1)
            lane = row + jnp.where(upper, rows, 0)
            mask = lax.broadcasted_iota(I32, (cells, padded), 0) == cell
            values = [split(force[k, m, :], 2) for k in range(3)]
            left = jnp.concatenate(
                [jnp.where(mask, values[k][part], 0.0) for part in range(2) for k in range(3)], axis=0
            ).astype(BF16)
            right = jnp.where(
                lax.broadcasted_iota(I32, (2 * rows, padded), 0) == lane, 1.0, 0.0
            ).astype(BF16)
            product = lax.dot_general(left, right, NT, preferred_element_type=F32)
            running = product if running is None else running + product
        acc[...] += running

    for k in range(3):
        value = acc[k * cells : (k + 1) * cells] + acc[(3 + k) * cells : (4 + k) * cells]
        halves = []
        for part in range(2):
            b = value[:, part * rows : (part + 1) * rows]
            halves.append(0.5 * b + 0.25 * (pltpu.roll(b, 1, 1) + pltpu.roll(b, rows - 1, 1)))
        smooth = []
        for p in range(plane_count + 2):
            b = jnp.concatenate([h[p * half : (p + 1) * half] for h in halves], axis=0)
            smooth.append(
                0.5 * b[1 : columns + 1] + 0.25 * (b[:columns] + b[2 : columns + 2])
            )
        for j in range(planes):
            total_plane = jnp.zeros((columns, rows), F32)
            for source, w in ((j - 2, 0.25), (j - 1, 0.5), (j, 0.25)):
                if 0 <= source < plane_count + 2:
                    total_plane = total_plane + w * smooth[source]
            out_ref[k, j] = total_plane


def equilibrium_pairs(density, velocity):
    squared = velocity[0] * velocity[0] + velocity[1] * velocity[1] + velocity[2] * velocity[2]
    base = 1.0 - 1.5 * squared
    result = [None] * 19
    result[0] = LATTICE_WEIGHTS[0] * density * base
    scaled = {w: w * density for w in (1.0 / 18.0, 1.0 / 36.0)}
    for q in range(1, 19, 2):
        projected = None
        for c, v in zip(LATTICE_VECTORS[q], velocity):
            if c == 0:
                continue
            if projected is None:
                projected = v if c == 1 else -v
            else:
                projected = projected + v if c == 1 else projected - v
        even = base + 4.5 * projected * projected
        odd = 3.0 * projected
        weight = scaled[LATTICE_WEIGHTS[q]]
        result[q] = weight * (even + odd)
        result[q + 1] = weight * (even - odd)
    return result


def moments_of(fields):
    density = functools.reduce(lambda a, b: a + b, fields)
    momentum = []
    for k in range(3):
        plus = [fields[q] for q in range(19) if LATTICE_VECTORS[q][k] == 1]
        minus = [fields[q] for q in range(19) if LATTICE_VECTORS[q][k] == -1]
        momentum.append(functools.reduce(lambda a, b: a + b, [a - b for a, b in zip(plus, minus)]))
    return density, momentum


def moving(dim, sign):
    return [q for q in range(19) if LATTICE_VECTORS[q][dim] == sign]


def lattice_kernel(
    slabs, crosses,
    tri_hbm, pos_hbm, ten_hbm, coarse_hbm, face_hbm, relax_hbm, fluid_hbm, pop_hbm,
    next_ref,
    tri_ref, pos_ref, ten_ref, coarse_ref, face_ref, relax_ref, fluid_ref, pop_ref,
    xs, inc, nodal, acc, force_ref,
    relaxed, pushed, rim, used_ref, coarse_all, parts,
    force_in, zsend, zrecv, xsend, xrecv, csend, crecv,
    load_sems, coarse_sems, force_sems, send_sems, recv_sems,
):
    _, plane_count, columns, rows = pop_ref.shape
    slab = lax.axis_index("slab")
    cross = lax.axis_index("cross")

    def beside(direction, sign):
        dz, dx = direction[0] * sign, direction[1] * sign
        conditions = []
        if dz == 1:
            conditions.append(slab < slabs - 1)
        if dz == -1:
            conditions.append(slab > 0)
        if dx == 1:
            conditions.append(cross < crosses - 1)
        if dx == -1:
            conditions.append(cross > 0)
        return functools.reduce(jnp.logical_and, conditions)

    def target(direction):
        return {"slab": slab + direction[0], "cross": cross + direction[1]}

    loads = [
        pltpu.make_async_copy(source, sink, load_sems.at[i])
        for i, (source, sink) in enumerate(
            (
                (tri_hbm, tri_ref),
                (pos_hbm, pos_ref),
                (ten_hbm, ten_ref),
                (coarse_hbm, coarse_ref),
                (face_hbm, face_ref),
                (relax_hbm, relax_ref),
                (fluid_hbm, fluid_ref),
                (pop_hbm, pop_ref),
            )
        )
    ]
    for load in loads:
        load.start()

    force_in[...] = jnp.zeros_like(force_in)
    zrecv[...] = jnp.zeros_like(zrecv)
    xrecv[...] = jnp.zeros_like(xrecv)
    crecv[...] = jnp.zeros_like(crecv)
    parts[...] = jnp.zeros_like(parts)

    barrier = pltpu.get_barrier_semaphore()

    @pl.loop(1, slabs)
    def _(d):
        peer = lax.rem(slab + d, slabs)
        pl.semaphore_signal(
            barrier, inc=1, device_id={"slab": peer, "cross": cross}, device_id_type=MESH
        )

    expected = slabs - 1
    for direction in DIRECTIONS:
        if direction[1] == 0:
            continue
        there = beside(direction, 1)
        expected = expected + jnp.where(there, 1, 0)

        @pl.when(there)
        def _():
            pl.semaphore_signal(
                barrier, inc=1, device_id=target(direction), device_id_type=MESH
            )

    for load in loads[:3]:
        load.wait()
    nodal_stage(plane_count, columns, rows, pos_ref, tri_ref, ten_ref, xs, inc, nodal)
    loads[3].wait()
    pl.semaphore_wait(barrier, expected)
    coarse_all[slab] = coarse_ref[...]

    def coarse_copy(d):
        return pltpu.make_async_remote_copy(
            src_ref=coarse_ref,
            dst_ref=coarse_all.at[slab],
            send_sem=coarse_sems.at[0, d],
            recv_sem=coarse_sems.at[1, d],
            device_id={"slab": lax.rem(slab + d, slabs), "cross": cross},
            device_id_type=MESH,
        )

    @pl.loop(1, slabs)
    def _(d):
        coarse_copy(d).start()

    spread_stage(xs, nodal, acc, force_ref)

    def force_copy(index):
        start = plane_count + 2 if index == 0 else 0
        return pltpu.make_async_remote_copy(
            src_ref=force_ref.at[:, pl.ds(start, 2)],
            dst_ref=force_in.at[index],
            send_sem=force_sems.at[0, index],
            recv_sem=force_sems.at[1, index],
            device_id=target(DIRECTIONS[index]),
            device_id_type=MESH,
        )

    for index in range(2):

        @pl.when(beside(DIRECTIONS[index], 1))
        def _():
            force_copy(index).start()

    for load in loads[4:]:
        load.wait()

    cell = face_ref[pl.ds(0, 1), :]
    slots = cell.shape[1]
    used = cell >= 0
    place = jnp.where(used, cell // rows, -1)
    lane = jnp.where(used, cell % rows, -1)
    first = face_ref[pl.ds(1, 1), :]
    second = face_ref[pl.ds(2, 1), :]
    width = coarse_ref.shape[1]

    @pl.loop(1, slabs)
    def _(d):
        pltpu.make_async_remote_copy(
            src_ref=coarse_ref,
            dst_ref=coarse_all.at[lax.rem(slab + slabs - d, slabs)],
            send_sem=coarse_sems.at[0, d],
            recv_sem=coarse_sems.at[1, d],
            device_id={"slab": lax.rem(slab + d, slabs), "cross": cross},
            device_id_type=MESH,
        ).wait_recv()

    def blend(j, running):
        for i, piece in enumerate(split(coarse_all[j], 3)):
            parts[pl.ds(8 * i, 4), :] = piece
        ids = lax.broadcasted_iota(I32, (width, slots), 0) + j * width
        table = jnp.where(ids == first, 0.75, 0.0) + jnp.where(ids == second, 0.25, 0.0)
        return running + jnp.dot(
            parts[...].astype(BF16), table.astype(BF16), preferred_element_type=F32
        )

    mixed = lax.fori_loop(0, slabs, blend, jnp.zeros((24, slots), F32))
    blended = mixed[0:4] + (mixed[8:12] + mixed[16:20])

    cells = plane_count * columns
    mask = lax.broadcasted_iota(I32, (cells, slots), 0) == place
    pieces = split(blended, 3)
    left = [jnp.where(mask, piece[m : m + 1], 0.0) for m in range(4) for piece in pieces]
    left.append(jnp.where(mask, 1.0, 0.0))
    right = jnp.where(lax.broadcasted_iota(I32, (rows, slots), 0) == lane, 1.0, 0.0)
    placed = lax.dot_general(
        jnp.concatenate(left, axis=0).astype(BF16), right.astype(BF16), NT, preferred_element_type=F32
    )

    def placed_at(index, p):
        start = index * cells + p * columns
        return placed[start : start + columns]

    for p in range(plane_count):
        filled = [
            placed_at(3 * m, p) + (placed_at(3 * m + 1, p) + placed_at(3 * m + 2, p)) for m in range(4)
        ]
        used_ref[p] = placed_at(12, p)
        for q, value in enumerate(equilibrium_pairs(filled[0], filled[1:])):
            rim[q, p] = value

    for index in range(2):

        @pl.when(beside(DIRECTIONS[index], -1))
        def _():
            force_copy(index).wait_recv()

    for k in range(3):
        for p in range(plane_count):
            value = force_ref[k, p + 2]
            if p < 2:
                value = value + force_in[0, k, p]
            if p >= plane_count - 2:
                value = value + force_in[1, k, p - plane_count + 2]
            pushed[k, p] = value / relax_ref[p]

    sublane = lax.broadcasted_iota(I32, (columns, rows), 0)
    ups, downs = moving(0, 1), moving(0, -1)
    rights, lefts = moving(1, 1), moving(1, -1)
    corner_of = {7: 0, 8: 1, 9: 2, 10: 3}

    def halo_copy(step, index):
        if index < 2:
            source, sink = zsend.at[step, index], zrecv.at[step, index]
        elif index < 4:
            source, sink = xsend.at[step, index - 2], xrecv.at[step, index - 2]
        else:
            source, sink = csend.at[step, index - 4], crecv.at[step, index - 4]
        return pltpu.make_async_remote_copy(
            src_ref=source,
            dst_ref=sink,
            send_sem=send_sems.at[step % 2, index],
            recv_sem=recv_sems.at[step % 2, index],
            device_id=target(DIRECTIONS[index]),
            device_id_type=MESH,
        )

    for step in range(STEPS):
        fields_ref = pop_ref if step == 0 else next_ref
        for p in range(plane_count):
            fields = [fields_ref[q, p] for q in range(19)]
            density, momentum = moments_of(fields)
            inverse = 1.0 / density
            shifted = [(momentum[k] + pushed[k, p]) * inverse for k in range(3)]
            rate = relax_ref[p]
            fluid = fluid_ref[p] == 1
            for q, goal in enumerate(equilibrium_pairs(density, shifted)):
                value = fields[q] + rate * (goal - fields[q])
                value = jnp.where(fluid, value, fields[OPPOSITE[q]])
                relaxed[q, p] = value
                if p == plane_count - 1 and q in ups:
                    zsend[step, 0, ups.index(q)] = value
                if p == 0 and q in downs:
                    zsend[step, 1, downs.index(q)] = value
                if q in rights:
                    xsend[step, 0, rights.index(q), p : p + 1] = value[columns - 1 :]
                if q in lefts:
                    xsend[step, 1, lefts.index(q), p : p + 1] = value[:1]
                if q in corner_of:
                    cz, cx, _ = LATTICE_VECTORS[q]
                    if p == (plane_count - 1 if cz == 1 else 0):
                        edge = value[columns - 1 :] if cx == 1 else value[:1]
                        csend[step, corner_of[q]] = edge
        for index in (4, 5, 6, 7, 0, 1, 2, 3):

            @pl.when(beside(DIRECTIONS[index], 1))
            def _():
                if step >= 2:
                    halo_copy(step - 2, index).wait_send()
                halo_copy(step, index).start()

        for index in range(8):

            @pl.when(beside(DIRECTIONS[index], -1))
            def _():
                halo_copy(step, index).wait_recv()

        for p in range(plane_count):
            fixed = used_ref[p] > 0.5
            for q, (cz, cx, cy) in enumerate(LATTICE_VECTORS):
                source = p - cz
                within = 0 <= source < plane_count
                if within:
                    value = relaxed[q, source]
                elif cz == 1:
                    value = zrecv[step, 0, ups.index(q)]
                else:
                    value = zrecv[step, 1, downs.index(q)]
                if cx != 0:
                    side, members = (0, rights) if cx == 1 else (1, lefts)
                    if within:
                        edge = xrecv[step, side, members.index(q), source : source + 1]
                    else:
                        edge = crecv[step, corner_of[q]]
                    value = pltpu.roll(value, cx % columns, 0)
                    at = 0 if cx == 1 else columns - 1
                    value = jnp.where(sublane == at, edge, value)
                if cy != 0:
                    value = pltpu.roll(value, cy % rows, 1)
                next_ref[q, p] = jnp.where(fixed, rim[q, p], value)

    @pl.loop(1, slabs)
    def _(d):
        coarse_copy(d).wait_send()

    for index in range(2):

        @pl.when(beside(DIRECTIONS[index], 1))
        def _():
            force_copy(index).wait_send()

    for index in range(8):

        @pl.when(beside(DIRECTIONS[index], 1))
        def _():
            for step in range(max(0, STEPS - 2), STEPS):
                halo_copy(step, index).wait_send()


def flow_kernel(fields_ref, next_ref, flow_ref):
    for p in range(fields_ref.shape[1]):
        fields = [fields_ref[q, p] for q in range(19)]
        for q, value in enumerate(fields):
            next_ref[q, p] = value
        density, momentum = moments_of(fields)
        inverse = ROOT_THREE / density
        for k in range(3):
            flow_ref[k, p] = momentum[k] * inverse


def on_device(
    slabs, crosses,
    populations, fluid_mask, relaxation, positions, triangles, tension, coarse_moments, interface,
):
    _, plane_count, columns, rows = populations.shape
    _, membranes, nodes = positions.shape
    padded = round_up(nodes, 128)
    corners = triangles.shape[1]
    half = (columns + 2) // 2
    cells = round_up((plane_count + 2) * half, 16)
    vmem = pl.BlockSpec(memory_space=pltpu.VMEM)
    block = (19, plane_count, columns, rows)
    operands = (
        triangles, positions, tension, coarse_moments, interface, relaxation, fluid_mask, populations,
    )
    fields = pl.pallas_call(
        functools.partial(lattice_kernel, slabs, crosses),
        name="lattice_steps",
        out_shape=jax.ShapeDtypeStruct(block, F32),
        in_specs=[pl.BlockSpec(memory_space=pl.ANY)] * 8,
        out_specs=vmem,
        scratch_shapes=[pltpu.VMEM(operand.shape, operand.dtype) for operand in operands]
        + [
            pltpu.VMEM((3, membranes, padded), F32),
            pltpu.VMEM((padded, corners), BF16),
            pltpu.VMEM((3, membranes, padded), F32),
            pltpu.VMEM((6 * cells, 2 * rows), F32),
            pltpu.VMEM((3, plane_count + 4, columns, rows), F32),
            pltpu.VMEM(block, F32),
            pltpu.VMEM((3,) + block[1:], F32),
            pltpu.VMEM(block, F32),
            pltpu.VMEM(block[1:], F32),
            pltpu.VMEM((slabs,) + coarse_moments.shape, F32),
            pltpu.VMEM((24, coarse_moments.shape[1]), F32),
            pltpu.VMEM((2, 3, 2, columns, rows), F32),
            pltpu.VMEM((STEPS, 2, 5, columns, rows), F32),
            pltpu.VMEM((STEPS, 2, 5, columns, rows), F32),
            pltpu.VMEM((STEPS, 2, 5, plane_count, rows), F32),
            pltpu.VMEM((STEPS, 2, 5, plane_count, rows), F32),
            pltpu.VMEM((STEPS, 4, 1, rows), F32),
            pltpu.VMEM((STEPS, 4, 1, rows), F32),
            pltpu.SemaphoreType.DMA((8,)),
            pltpu.SemaphoreType.DMA((2, slabs)),
            pltpu.SemaphoreType.DMA((2, 2)),
            pltpu.SemaphoreType.DMA((2, 8)),
            pltpu.SemaphoreType.DMA((2, 8)),
        ],
        compiler_params=pltpu.CompilerParams(collective_id=0, has_side_effects=True),
    )(*operands)
    return pl.pallas_call(
        flow_kernel,
        name="flow",
        out_shape=(
            jax.ShapeDtypeStruct(block, F32),
            jax.ShapeDtypeStruct((3,) + block[1:], F32),
        ),
        in_specs=[vmem],
        out_specs=(vmem, vmem),
    )(fields)


def solution(mesh):
    in_specs = (
        P(None, "slab", "cross", None),
        P("slab", "cross", None),
        P("slab", "cross", None),
        P(None, "slab", None),
        P(),
        P("slab", None),
        P(None, "slab"),
        P(None, ("slab", "cross")),
    )
    out_specs = (P(None, "slab", "cross", None), P(None, "slab", "cross", None))
    return jax.shard_map(
        functools.partial(on_device, mesh.shape["slab"], mesh.shape["cross"]),
        mesh=mesh, in_specs=in_specs, out_specs=out_specs, check_vma=False,
    )
```
